32 devices in a mesh: ctx: 8 (over z, core), tp: 4 (over y, x).
Axes of the slice: x: 2, y: 2, z: 4, core: 2. Of those that a mesh axis runs over, the one named last changes fastest.
Arguments:
- tokens: bfloat16 [2, 4096, 8192], P(None, 'ctx', 'tp'), may hold values from -14 to 14
- norm_gain: float32 [8192], replicated, may hold values from 0.5 to 1.5
- span_order: int32 [2, 16], replicated, may hold values from 0 to 15, each once within a row
- w_query: bfloat16 [8192, 4096], P('ctx', 'tp'), may hold values from -0.10122281 to 0.10122281
- w_key: bfloat16 [8192, 1024], P('ctx', 'tp'), may hold values from -0.10122281 to 0.10122281
- value_weight: bfloat16 [8192, 1024], P('ctx', 'tp'), may hold values from -0.0625 to 0.0625
- w_out: bfloat16 [4096, 8192], P('tp', 'ctx'), may hold values from -0.75 to 0.75
Outputs:
- mixed: bfloat16 [2, 4096, 8192], P(None, 'ctx', 'tp')
The draws below stay inside these ranges and needn't reach their ends.
Inputs may be any that keep to these rules, and one draw needn't show every extreme that they name: Each row of span_order names every one of the 2 * 8 blocks of positions once; stored block b of a sequence holds positions span_order[b] * 256 onwards, in order.
All inputs are finite; a program needn't handle non-finite values.
Results may differ from the reference program's by a relative error of at most 0.014.
Values may be sent and summed in bfloat16 or wider, within the bound.
A program may use at most 128 MiB of HBM per device.

```python
import math
import jax
import jax.numpy as jnp
from jax import lax

MODEL_WIDTH = 8192
QUERY_HEAD_COUNT = 32
KEY_VALUE_HEADS = 8
HEAD_DIM = 128
SEQUENCE_LENGTH = 4096
SEQS = 2
N_CTX = 8
N_TP = 4


def unscaled_weight(key, salt, columns):
    spread = (2.0 / MODEL_WIDTH) ** 0.5
    normal_part = jax.random.normal(jax.random.fold_in(key, salt), (MODEL_WIDTH, columns), jnp.float32)
    return jnp.clip(normal_part, -6.0, 6.0) * spread


def draw_w_query(key, part):
    weight_portion = unscaled_weight(key, 11, QUERY_HEAD_COUNT * HEAD_DIM)
    return weight_portion.astype(jnp.bfloat16)


def draw_w_key(key, part):
    weight_portion = unscaled_weight(key, 12, KEY_VALUE_HEADS * HEAD_DIM)
    return weight_portion.astype(jnp.bfloat16)


def draw_tokens(key, part):
    noise_part = jnp.clip(jax.random.normal(jax.random.fold_in(key, 13), (SEQS, SEQUENCE_LENGTH, MODEL_WIDTH), jnp.float32), -6.0, 6.0)
    return noise_part.astype(jnp.bfloat16)


def level_of(key, extent, cuts, smallest, high):
    loudness = 1.0
    for axis_at, parts in cuts:
        draws = jax.random.uniform(jax.random.fold_in(jax.random.fold_in(key, 6), axis_at), (parts,), jnp.float32, smallest / len(cuts), high / len(cuts))
        loudness = loudness * jnp.repeat(jnp.exp(draws), extent[axis_at] // parts).reshape((-1,) + (1,) * (len(extent) - 1 - axis_at))
    return loudness


def noise(rng, shape, deviation, reach, cuts=(), kind=jnp.bfloat16):
    array = deviation * jax.random.normal(rng, shape, jnp.float32)
    if cuts:
        array = array * level_of(rng, shape, cuts, -0.22, 0.18)
    return jnp.clip(array, -reach, reach).astype(kind)


def setup_inputs(seed: int = 0) -> dict:
    splits = jax.random.split(jax.random.key(seed), 8)
    return {
        "tokens": draw_tokens(jax.random.fold_in(splits[7], 71), 0),
        "norm_gain": jnp.clip(1.0 + 0.1 * jax.random.normal(splits[1], (MODEL_WIDTH,), jnp.float32), 0.5, 1.5),
        "span_order": jax.vmap(lambda own: jax.random.permutation(own, 2 * N_CTX))(jax.random.split(splits[2], SEQS)).reshape((SEQS, 2 * N_CTX)).astype(jnp.int32),
        "w_query": draw_w_query(jax.random.fold_in(splits[7], 71), 0),
        "w_key": draw_w_key(jax.random.fold_in(splits[7], 71), 0),
        "value_weight": noise(splits[5], (MODEL_WIDTH, KEY_VALUE_HEADS * HEAD_DIM), MODEL_WIDTH ** -0.5, 0.0625, ((0, 8), (1, 4))),
        "w_out": noise(splits[6], (QUERY_HEAD_COUNT * HEAD_DIM, MODEL_WIDTH), (QUERY_HEAD_COUNT * HEAD_DIM // 64) ** -0.5, 0.75, ((0, 4), (1, 8))),
    }


theta_base = 500000.0
norm_eps = 1e-05
masked_score = -1e+30

def normalize(flat_rows, norm_gain):
    wide = flat_rows.astype(jnp.float32)
    factor = lax.rsqrt(lax.optimization_barrier(jnp.mean(wide * wide, axis=-1, keepdims=True)) + norm_eps)
    return (wide * factor * norm_gain).astype(jnp.bfloat16)

def positions_of(span_order, first, count, block_rows):
    stored = first + jnp.arange(count, dtype=jnp.int32)
    which = stored // block_rows
    slots = jnp.arange(span_order.shape[1], dtype=jnp.int32)
    picked = lax.optimization_barrier(jnp.sum(jnp.where(slots[None, None, :] == which[None, :, None], span_order[:, None, :], 0), axis=2))
    return (picked * block_rows + stored % block_rows).astype(jnp.int32)

def apply_rotation(value_rows, token_position, head_size):
    half = head_size // 2
    freqs = jnp.exp(-(2.0 * jnp.arange(half, dtype=jnp.float32) / head_size) * math.log(theta_base))
    angle = token_position.astype(jnp.float32)[..., None] * freqs
    cosine = jnp.cos(angle)[:, :, None, :]
    sine = jnp.sin(angle)[:, :, None, :]
    front = value_rows[..., :half]
    back = value_rows[..., half:]
    return jnp.concatenate([front * cosine - back * sine, back * cosine + front * sine], axis=-1)

def reference(tokens, norm_gain, span_order, w_query, w_key, value_weight, w_out):
    sequence_batch = tokens.shape[0]
    token_length = tokens.shape[1]
    block_rows = token_length // (2 * N_CTX)
    normed = normalize(tokens.reshape(sequence_batch * token_length, MODEL_WIDTH), norm_gain)
    token_position = positions_of(span_order, 0, token_length, block_rows)
    query_flat = jnp.dot(normed, w_query, preferred_element_type=jnp.float32)
    flattened_key = jnp.dot(normed, w_key, preferred_element_type=jnp.float32)
    flattened_value = jnp.dot(normed, value_weight, preferred_element_type=jnp.float32)
    query = apply_rotation(query_flat.reshape(sequence_batch, token_length, QUERY_HEAD_COUNT, HEAD_DIM), token_position, HEAD_DIM).astype(jnp.bfloat16)
    key_rows = apply_rotation(flattened_key.reshape(sequence_batch, token_length, KEY_VALUE_HEADS, HEAD_DIM), token_position, HEAD_DIM).astype(jnp.bfloat16)
    value_rows = flattened_value.reshape(sequence_batch, token_length, KEY_VALUE_HEADS, HEAD_DIM).astype(jnp.bfloat16)
    group_width = QUERY_HEAD_COUNT // KEY_VALUE_HEADS
    factor = 1.0 / math.sqrt(HEAD_DIM)
    allowed = token_position[:, None, :] <= token_position[:, :, None]

    def single_head(head):
        query_block = lax.dynamic_slice_in_dim(query, (head * group_width).astype(jnp.int32), group_width, 2).astype(jnp.float32)
        key_block = lax.dynamic_slice_in_dim(key_rows, head.astype(jnp.int32), 1, 2)[:, :, 0, :].astype(jnp.float32)
        value_block = lax.dynamic_slice_in_dim(value_rows, head.astype(jnp.int32), 1, 2)[:, :, 0, :].astype(jnp.float32)
        scores = jnp.einsum('sqgd,skd->sgqk', query_block, key_block) * factor
        scores = jnp.where(allowed[:, None], scores, masked_score)
        peak = lax.optimization_barrier(jnp.max(scores, axis=-1, keepdims=True))
        weights = jnp.where(allowed[:, None], jnp.exp(scores - peak), 0.0)
        total = lax.optimization_barrier(jnp.sum(weights, axis=-1))
        rounded = lax.optimization_barrier(weights.astype(jnp.bfloat16)).astype(jnp.float32)
        summed = jnp.einsum('sgqk,skd->sqgd', rounded, value_block)
        return (summed / jnp.transpose(total, (0, 2, 1))[..., None]).astype(jnp.bfloat16)
    head_outputs = lax.map(single_head, jnp.arange(KEY_VALUE_HEADS, dtype=jnp.int32))
    attended = jnp.transpose(head_outputs, (1, 2, 0, 3, 4)).reshape(sequence_batch * token_length, QUERY_HEAD_COUNT * HEAD_DIM)
    columns = QUERY_HEAD_COUNT * HEAD_DIM // N_TP
    summed = jnp.zeros((sequence_batch * token_length, MODEL_WIDTH), jnp.float32)
    for group in range(N_TP):
        partial_value = jnp.dot(attended[:, group * columns:(group + 1) * columns], w_out[group * columns:(group + 1) * columns], preferred_element_type=jnp.float32)
        summed = summed + lax.optimization_barrier(partial_value.astype(jnp.bfloat16)).astype(jnp.float32)
    return summed.astype(jnp.bfloat16).reshape(sequence_batch, token_length, MODEL_WIDTH)
```

```python
import functools
import math

import jax
import jax.numpy as jnp
from jax import lax
from jax.experimental import pallas as pl
from jax.experimental.pallas import tpu as pltpu
from jax.sharding import PartitionSpec as P

HEAD_DIM = 128


theta_base = 500000.0
norm_eps = 1e-05
masked_score = -1e30


def normalize(flat_rows, norm_gain):
    wide = flat_rows.astype(jnp.float32)
    factor = lax.rsqrt(jnp.mean(wide * wide, axis=-1, keepdims=True) + norm_eps)
    return (wide * factor * norm_gain).astype(jnp.bfloat16)


def positions_of(span_order, first, count, block_rows):
    stored = first + jnp.arange(count, dtype=jnp.int32)
    which = stored // block_rows
    slots = jnp.arange(span_order.shape[1], dtype=jnp.int32)
    picked = jnp.sum(
        jnp.where(slots[None, None, :] == which[None, :, None], span_order[:, None, :], 0), axis=2
    )
    return picked * block_rows + stored % block_rows


def apply_rotation(value_rows, cosine, sine):
    half = value_rows.shape[-1] // 2
    front = value_rows[..., :half]
    back = value_rows[..., half:]
    return jnp.concatenate([front * cosine - back * sine, back * cosine + front * sine], axis=-1)


def gather_kernel(n, count, *refs):
    ins, outs, stages = refs[:count], refs[count : 2 * count], refs[2 * count : 3 * count]
    load_sem, keep_sem, own_send, own_recv, ring_send, ring_recv, near_send, near_recv = refs[3 * count :]
    chips = n // 2
    me = lax.axis_index("ctx")
    chip, core = me // 2, me % 2
    right = lax.rem(chip + 1, chips) * 2 + core
    left = lax.rem(chip + chips - 1, chips) * 2 + core
    near = chip * 2 + 1 - core
    towards = (right, left)

    barrier = pltpu.get_barrier_semaphore()
    for other in (right, left, near):
        pl.semaphore_signal(
            barrier, inc=1, device_id={"ctx": other}, device_id_type=pl.DeviceIdType.MESH
        )
    pl.semaphore_wait(barrier, 3)

    def remote(source, target, send, recv, other):
        return pltpu.make_async_remote_copy(
            src_ref=source,
            dst_ref=target,
            send_sem=send,
            recv_sem=recv,
            device_id={"ctx": other},
            device_id_type=pl.DeviceIdType.MESH,
        )

    def region(a, owner, h):
        length = ins[a].shape[0]
        return outs[a].at[pl.ds(owner * length + h * (length // 2), length // 2)]

    def whole(a, owner):
        length = ins[a].shape[0]
        return outs[a].at[pl.ds(owner * length, length)]

    loads = []
    for a in range(count):
        loads.append(pltpu.make_async_copy(ins[a], stages[a], load_sem.at[a]))
        loads[a].start()
    started, kept = [], []
    for a in range(count):
        loads[a].wait()
        for h in range(2):
            length = ins[a].shape[0] // 2
            slot = (a * 2 + h) * (chips - 1)
            copy = remote(
                stages[a].at[pl.ds(h * length, length)],
                region(a, me, h),
                ring_send.at[slot],
                ring_recv.at[slot],
                towards[h],
            )
            copy.start()
            started.append(copy)
        copy = remote(stages[a], whole(a, me), own_send.at[a], own_recv.at[a], near)
        copy.start()
        started.append(copy)
        keep = pltpu.make_async_copy(stages[a], whole(a, me), keep_sem.at[a])
        keep.start()
        kept.append(keep)

    for step in range(1, chips):
        for a in range(count):
            for h in range(2):
                turn = chips - step if h == 0 else step
                owner = lax.rem(chip + turn, chips) * 2 + core
                piece = region(a, owner, h)
                slot = (a * 2 + h) * (chips - 1) + step - 1
                remote(
                    piece, piece, ring_send.at[slot], ring_recv.at[slot], towards[h]
                ).wait_recv()
                if step < chips - 1:
                    copy = remote(
                        piece, piece, ring_send.at[slot + 1], ring_recv.at[slot + 1], towards[h]
                    )
                    copy.start()
                    started.append(copy)
                copy = remote(piece, piece, near_send.at[slot], near_recv.at[slot], near)
                copy.start()
                started.append(copy)

    for a in range(count):
        kept[a].wait()
        remote(stages[a], whole(a, near), own_send.at[a], own_recv.at[a], near).wait_recv()
        for step in range(1, chips):
            for h in range(2):
                turn = chips - step if h == 0 else step
                owner = lax.rem(chip + turn, chips) * 2 + 1 - core
                piece = region(a, owner, h)
                slot = (a * 2 + h) * (chips - 1) + step - 1
                remote(piece, piece, near_send.at[slot], near_recv.at[slot], near).wait_recv()
    for copy in started:
        copy.wait_send()


def gather_ctx(arrays, n, ident, micros):
    count = len(arrays)
    slots = count * 2 * (n // 2 - 1)
    moved = sum(a.size * a.dtype.itemsize for a in arrays) * n
    dma = pltpu.SemaphoreType.DMA
    return pl.pallas_call(
        functools.partial(gather_kernel, n, count),
        out_shape=tuple(
            jax.ShapeDtypeStruct((n * a.shape[0],) + a.shape[1:], a.dtype) for a in arrays
        ),
        in_specs=[pl.BlockSpec(memory_space=pl.ANY)] * count,
        out_specs=(pl.BlockSpec(memory_space=pl.ANY),) * count,
        scratch_shapes=[pltpu.VMEM(a.shape, a.dtype) for a in arrays]
        + [dma((count,))] * 4
        + [dma((slots,))] * 4,
        compiler_params=pltpu.CompilerParams(collective_id=ident, has_side_effects=True),
        cost_estimate=pl.CostEstimate(
            flops=int(micros * 9e8), bytes_accessed=moved, transcendentals=0
        ),
        name=f"gather_ctx_{ident}",
    )(*arrays)


def attention_kernel(blocks, group, sequence, span_ref, q_ref, k_ref, v_ref, o_ref, peak_ref, total_ref, sum_ref):
    rows = q_ref.shape[2]
    rank = lax.axis_index("ctx")
    own = rank * 2 + pl.program_id(1)
    own_place = span_ref[sequence, own]

    def scores_of(g, keys):
        return lax.dot_general(
            q_ref[0, g], keys, (((1,), (1,)), ((), ())), preferred_element_type=jnp.float32
        )

    def load(ref, index):
        first = pl.multiple_of((index % 2) * rows, rows)
        return ref[index // 2, 0, 0, 0, pl.ds(first, rows), :]

    def folded(weights):
        parts = [weights[:, i : i + 128] for i in range(0, weights.shape[1], 128)]
        return functools.reduce(jnp.add, parts)

    keys, vals = load(k_ref, own), load(v_ref, own)
    allowed = lax.broadcasted_iota(jnp.int32, (rows, rows), 1) <= lax.broadcasted_iota(
        jnp.int32, (rows, rows), 0
    )
    for g in range(group):
        scores = jnp.where(allowed, scores_of(g, keys), masked_score)
        peak = jnp.max(scores, axis=1, keepdims=True)
        weights = jnp.where(allowed, jnp.exp2(scores - peak), 0.0)
        peak_ref[g] = jnp.broadcast_to(peak, (rows, 128))
        total_ref[g] = folded(weights)
        sum_ref[g] = jnp.dot(weights.astype(jnp.bfloat16), vals, preferred_element_type=jnp.float32)

    def visit(index, carry):
        @pl.when(span_ref[sequence, index] < own_place)
        def _():
            keys, vals = load(k_ref, index), load(v_ref, index)
            for g in range(group):
                scores = scores_of(g, keys)
                old = peak_ref[g][:, :1]
                peak = jnp.maximum(old, jnp.max(scores, axis=1, keepdims=True))
                weights = jnp.exp2(scores - peak)
                shrink = jnp.exp2(old - peak)
                peak_ref[g] = jnp.broadcast_to(peak, (rows, 128))
                total_ref[g] = total_ref[g] * shrink + folded(weights)
                sum_ref[g] = sum_ref[g] * shrink + jnp.dot(
                    weights.astype(jnp.bfloat16), vals, preferred_element_type=jnp.float32
                )

        return carry

    lax.fori_loop(0, blocks, visit, 0)
    for g in range(group):
        total = jnp.sum(total_ref[g], axis=1, keepdims=True)
        o_ref[:, g * HEAD_DIM : (g + 1) * HEAD_DIM] = (sum_ref[g] / total).astype(jnp.bfloat16)


def attend(span_order, query, pairs, sequence, n):
    key_heads, group, rows_dev, head_size = query.shape
    rows = rows_dev // 2
    pair_shape = (n, 1, 1, 1, rows_dev, head_size)
    flops = 2 * key_heads * group * rows_dev * rows_dev * n * head_size * 2
    return pl.pallas_call(
        functools.partial(attention_kernel, 2 * n, group, sequence),
        grid_spec=pltpu.PrefetchScalarGridSpec(
            num_scalar_prefetch=1,
            grid=(key_heads, 2),
            in_specs=[
                pl.BlockSpec((1, group, rows, head_size), lambda h, i, s: (h, 0, i, 0)),
                pl.BlockSpec(pair_shape, lambda h, i, s: (0, 0, sequence, h, 0, 0)),
                pl.BlockSpec(pair_shape, lambda h, i, s: (0, 1, sequence, h, 0, 0)),
            ],
            out_specs=pl.BlockSpec((rows, group * head_size), lambda h, i, s: (i, h)),
            scratch_shapes=[pltpu.VMEM((group, rows, 128), jnp.float32)] * 3,
        ),
        out_shape=jax.ShapeDtypeStruct((rows_dev, key_heads * group * head_size), jnp.bfloat16),
        cost_estimate=pl.CostEstimate(
            flops=flops * 3, bytes_accessed=pairs.size, transcendentals=0
        ),
        name=f"attend_{sequence}",
    )(span_order, query, pairs, pairs)


def per_device(n, tokens, norm_gain, span_order, w_query, w_key, value_weight, w_out):
    sequence_batch, rows_dev, _ = tokens.shape
    head_size = HEAD_DIM
    query_heads = w_query.shape[1] // head_size
    key_heads = w_key.shape[1] // head_size
    group_width = query_heads // key_heads
    block_rows = rows_dev // 2
    total_rows = sequence_batch * rows_dev
    factor = math.log2(math.e) / math.sqrt(head_size)
    rank = lax.axis_index("ctx")
    whole = lax.all_gather(tokens, "tp", axis=2, tiled=True)
    whole_query, whole_key, whole_value = gather_ctx((w_query, w_key, value_weight), n, 0, 120)
    whole, whole_query, whole_key, whole_value = lax.optimization_barrier(
        (whole, whole_query, whole_key, whole_value)
    )
    normed = normalize(whole.reshape(total_rows, whole.shape[2]), norm_gain)
    w_out, normed = lax.optimization_barrier((w_out, normed))
    out_pieces = lax.all_gather(w_out, "ctx", axis=0)
    query_pos = positions_of(span_order, rank * rows_dev, rows_dev, block_rows)
    half = head_size // 2
    freqs = jnp.exp(-(2.0 * jnp.arange(half, dtype=jnp.float32) / head_size) * math.log(theta_base))
    angle = query_pos.astype(jnp.float32)[..., None] * freqs
    cosine = jnp.cos(angle)[:, :, None, :]
    sine = jnp.sin(angle)[:, :, None, :]

    flattened_key = jnp.dot(normed, whole_key, preferred_element_type=jnp.float32)
    flattened_value = jnp.dot(normed, whole_value, preferred_element_type=jnp.float32)
    own_keys = apply_rotation(
        flattened_key.reshape(sequence_batch, rows_dev, key_heads, head_size), cosine, sine
    ).astype(jnp.bfloat16)
    own_values = flattened_value.reshape(sequence_batch, rows_dev, key_heads, head_size).astype(
        jnp.bfloat16
    )
    pair = jnp.stack([own_keys.transpose(0, 2, 1, 3), own_values.transpose(0, 2, 1, 3)])
    (pairs,) = gather_ctx((pair,), n, 1, 40)
    pairs = pairs.reshape((n, 2) + pair.shape[1:])

    query_flat = jnp.dot(normed, whole_query, preferred_element_type=jnp.float32)
    query = (
        apply_rotation(
            query_flat.reshape(sequence_batch, rows_dev, query_heads, head_size),
            cosine * factor,
            sine * factor,
        )
        .astype(jnp.bfloat16)
        .reshape(sequence_batch, rows_dev, key_heads, group_width, head_size)
        .transpose(0, 2, 3, 1, 4)
    )
    results = []
    for sequence in range(sequence_batch):
        attended = attend(span_order, query[sequence], pairs, sequence, n)
        terms = jnp.einsum(
            "rk,nkc->nrc", attended, out_pieces, preferred_element_type=jnp.float32
        ).astype(jnp.bfloat16)
        mixed = lax.psum_scatter(terms, "tp", scatter_dimension=0, tiled=True)
        results.append(mixed.transpose(1, 0, 2).reshape(rows_dev, -1))
    return jnp.stack(results)


def solution(mesh):
    placed = (
        P(None, "ctx", "tp"),
        P(),
        P(),
        P("ctx", "tp"),
        P("ctx", "tp"),
        P("ctx", "tp"),
        P("tp", "ctx"),
    )
    return jax.shard_map(
        functools.partial(per_device, mesh.shape["ctx"]),
        mesh=mesh,
        in_specs=placed,
        out_specs=P(None, "ctx", "tp"),
        check_vma=False,
    )
```
